32 devices in a mesh: blk: 4 (over y, x), in: 8 (over z, core).
Axes of the slice: x: 2, y: 2, z: 4, core: 2. Of those that a mesh axis runs over, the one named last changes fastest.
Arguments:
- heat_source: float32 [6144, 2048], P('blk', 'in'), may hold values from -6 to 6
- conductance: float32 [6144, 2048], P('blk', 'in'), may hold values from 0.1 to 2
- start_field: float32 [6144, 2048], P('blk', 'in'), may hold values from -6 to 8
- colour_map: int32 [2, 4], P(None, 'blk'), may hold values from 0 to 1
- projection: int32 [4, 2, 2048], P('blk', None, 'in'), may hold values from 0 to 2047
- face_counts: int32 [4, 2], P('blk'), may hold values from 1024 to 2048
Outputs:
- temperature: float32 [6144, 2048], P('blk', 'in')
- block_rms: float32 [4], P('blk')
The draws below stay inside these ranges and needn't reach their ends.
Inputs may be any that keep to these rules, and one draw needn't show every extreme that they name: `colour_map`: neighbouring blocks may share a colour.
All inputs are finite; a program needn't handle non-finite values.
Results may differ from the reference program's by a relative error of at most 0.00002.
Values sent between devices are 32-bit elements; how exact they have to be, the bound alone decides.
A program may use at most 64 MiB of HBM per device.

```python
import math
import jax
import jax.numpy as jnp
from jax import lax

NXB = 1536
SWEEPS = 2
INNER = 4
BLOCKS = 4
FACE = 2048
ROWS = 6144


def draw_start_field(key, part):
    noise = jax.random.normal(jax.random.fold_in(key, 31), (ROWS, FACE), jnp.float32)
    return jnp.clip(noise, -6.0, 6.0).astype(jnp.float32)


def draw_projection(key, part):
    ratio = jax.random.randint(jax.random.fold_in(key, 21), (BLOCKS, 2, 1), 3, 6)
    jitter = jax.random.randint(jax.random.fold_in(key, 22), (BLOCKS, 2, FACE), 0, 2)
    start = jax.random.randint(jax.random.fold_in(key, 23), (BLOCKS, 2, 1), 0, FACE // 4 + 1)
    base = jnp.arange(FACE, dtype=jnp.int32)[None, None, :]
    mapped = base * ratio // 4 + jitter + start - FACE // 8
    return jnp.clip(mapped, 0, FACE - 1).astype(jnp.int32)


def plant(entries, own_key, least, high):
    extent = entries.shape
    index_at = [jax.random.randint(jax.random.fold_in(own_key, axis), (), 0, extent[axis]) for axis in range(len(extent))]
    entries = entries.at[tuple(index_at)].set(least)
    longest = extent.index(max(extent))
    index_at[longest] = (index_at[longest] + 1) % extent[longest]
    return entries.at[tuple(index_at)].set(high)


def shard_levels(own_key, dims, split, smallest, top_value):
    loudness, own = 1.0, jax.random.fold_in(own_key, 6)
    for dim, shards_of in split:
        steps = jnp.exp(jax.random.uniform(jax.random.fold_in(own, dim), (shards_of,), jnp.float32, smallest / len(split), top_value / len(split)))
        loudness = loudness * jnp.repeat(steps, dims[dim] // shards_of).reshape([-1 if axis == dim else 1 for axis in range(len(dims))])
    return loudness


def bell_draw(own_key, dims, deviation, most, split=(), held_as=jnp.bfloat16):
    values = deviation * jax.random.normal(own_key, dims, jnp.float32)
    if split:
        values = values * shard_levels(own_key, dims, split, -0.22, 0.18)
    return jnp.clip(values, -most, most).astype(held_as)


def setup_inputs(seed: int = 0) -> dict:
    seeds = jax.random.split(jax.random.key(seed), 7)
    return {
        "heat_source": bell_draw(seeds[0], (ROWS, FACE), 1.0, 6.0, ((0, 4), (1, 8)), jnp.float32),
        "conductance": jnp.clip(jnp.exp(math.log(2.0) - 2.9957323 * jax.random.uniform(seeds[1], (ROWS, FACE), jnp.float32) ** shard_levels(seeds[1], (ROWS, FACE), ((0, 4), (1, 8)), -0.2, 0.2)), 0.1, 2.0),
        "start_field": draw_start_field(jax.random.fold_in(seeds[6], 71), 0),
        "colour_map": plant(jax.random.randint(seeds[3], (SWEEPS, BLOCKS), 0, 2), jax.random.fold_in(seeds[3], 1), 0, 1).astype(jnp.int32),
        "projection": draw_projection(jax.random.fold_in(seeds[6], 71), 0),
        "face_counts": plant(jax.random.randint(seeds[5], (BLOCKS, 2), FACE // 2, FACE + 1), jax.random.fold_in(seeds[5], 1), FACE // 2, FACE).astype(jnp.int32),
    }


def project_traces(field3, projection, face_counts):
    first_layer = field3[:, 0, :]
    last_layer = field3[:, -1, :]
    zero_layer = jnp.zeros((1, FACE), jnp.float32)
    from_left = jnp.concatenate([zero_layer, last_layer[:-1]], 0)
    from_right = jnp.concatenate([first_layer[1:], zero_layer], 0)
    position = jnp.arange(FACE, dtype=jnp.int32)[None, :]
    left_ghost = jnp.take_along_axis(from_left, projection[:, 0, :], axis=1) * (position < face_counts[:, 0:1]).astype(jnp.float32)
    right_ghost = jnp.take_along_axis(from_right, projection[:, 1, :], axis=1) * (position < face_counts[:, 1:2]).astype(jnp.float32)
    return (left_ghost, right_ghost)

def neighbour_sum(field3, left_ghost, right_ghost):
    x_before = jnp.concatenate([left_ghost[:, None, :], field3[:, :-1, :]], 1)
    x_after = jnp.concatenate([field3[:, 1:, :], right_ghost[:, None, :]], 1)
    zero_column = jnp.zeros((field3.shape[0], field3.shape[1], 1), jnp.float32)
    t_before = jnp.concatenate([zero_column, field3[:, :, :-1]], 2)
    t_after = jnp.concatenate([field3[:, :, 1:], zero_column], 2)
    return x_before + x_after + t_before + t_after

def reference(heat_source, conductance, start_field, colour_map, projection, face_counts):
    source3 = heat_source.reshape(BLOCKS, NXB, FACE)
    coeff3 = conductance.reshape(BLOCKS, NXB, FACE)
    inverse = 1.0 / (4.0 + coeff3)
    field = start_field.reshape(BLOCKS, NXB, FACE)
    for sweep_no in range(SWEEPS):
        for colour in (0, 1):
            left_ghost, right_ghost = project_traces(field, projection, face_counts)
            updated = field
            for step_no in range(INNER):
                updated = (source3 + neighbour_sum(updated, left_ghost, right_ghost)) * inverse
            field = jnp.where((colour_map[sweep_no] == colour)[:, None, None], updated, field)
    left_ghost, right_ghost = project_traces(field, projection, face_counts)
    residual = source3 - ((4.0 + coeff3) * field - neighbour_sum(field, left_ghost, right_ghost))
    block_rms = jnp.sqrt(lax.optimization_barrier(jnp.sum(residual * residual, axis=(1, 2))) / (NXB * FACE) + 1e-06)
    return (field.reshape(ROWS, FACE), block_rms)
```

```python
import functools

import jax
import jax.numpy as jnp
from jax import lax
from jax.experimental import pallas as pl
from jax.experimental.pallas import tpu as pltpu
from jax.sharding import PartitionSpec as P

SWEEPS = 2
INNER = 4
LANES = 128
SUB = 8
WINDOW = 16
STRIP = 32
CHUNK = 64
MESH = pl.DeviceIdType.MESH
F32 = jnp.float32


def shift_lanes(tiles, lane):
    n = len(tiles)
    fwd = [pltpu.roll(x, 1, 1) for x in tiles]
    back = [pltpu.roll(x, LANES - 1, 1) for x in tiles]
    left = [jnp.where(lane == 0, fwd[(t - 1) % n], fwd[t]) for t in range(n)]
    right = [jnp.where(lane == LANES - 1, back[(t + 1) % n], back[t]) for t in range(n)]
    return left, right


def kernel(
    nblk, nin, colour_ref, counts_ref, heat_hbm, cond_hbm, start_hbm, proj_ref,
    out_ref, rms_ref,
    va, vb, heat, cond, inv, pack, got, hedge, hproj, trace, seen, table, idx, ex, eh, ei,
    part, parts,
    load_sem, e_send, e_recv, h_send, h_recv, p_send, p_recv, s_send, s_recv,
):
    layers, width = start_hbm.shape
    tiles = width // LANES
    halo = tiles
    ntiles = tiles + 1
    blocks_of_rows = layers // LANES
    b = lax.axis_index("blk")
    k = lax.axis_index("in")
    before, after = lax.rem(b + nblk - 1, nblk), lax.rem(b + 1, nblk)
    lower, upper = lax.rem(k + nin - 1, nin), lax.rem(k + 1, nin)
    has_lower, has_upper = k > 0, k < nin - 1
    top = SUB
    last = SUB + layers - 1

    loads = []
    for a, (src, dst, off) in enumerate(
        ((start_hbm, va, SUB), (heat_hbm, heat, 0), (cond_hbm, cond, 0))
    ):
        for t in range(tiles):
            c = pltpu.make_async_copy(
                src.at[:, pl.ds(t * LANES, LANES)],
                dst.at[t, pl.ds(off, layers)],
                load_sem.at[a, t],
            )
            c.start()
            loads.append(c)

    barrier = pltpu.get_barrier_semaphore()

    def greet(i, _):
        for block in (before, after):
            pl.semaphore_signal(barrier, inc=1, device_id=(block, i), device_id_type=MESH)
        return 0

    def greet_own(i, _):
        pl.semaphore_signal(
            barrier, inc=1, device_id=(b, lax.rem(k + i, nin)), device_id_type=MESH
        )
        return 0

    lax.fori_loop(0, nin, greet, 0)
    lax.fori_loop(1, nin, greet_own, 0)

    zeros = jnp.zeros((SUB, LANES), F32)
    for v in (va, vb):
        for t in range(ntiles):
            v[t, pl.ds(0, SUB)] = zeros
            v[t, pl.ds(SUB + layers, SUB)] = zeros

    pl.semaphore_wait(barrier, 3 * nin - 1)

    def exchange(stage):
        def send(i, _):
            for side, block in ((0, after), (1, before)):
                pltpu.make_async_remote_copy(
                    src_ref=trace.at[stage, side],
                    dst_ref=seen.at[stage, side, k],
                    send_sem=e_send.at[stage],
                    recv_sem=e_recv.at[stage, side],
                    device_id=(block, i),
                    device_id_type=MESH,
                ).start()
            return 0

        lax.fori_loop(0, nin, send, 0)

    def bytes_of(ref, sem):
        pltpu.make_async_copy(ref, ref, sem).wait()

    for c in loads[:tiles]:
        c.wait()
    for t in range(tiles):
        trace[0, 0, pl.ds(t, 1)] = va[t, pl.ds(last, 1)]
        trace[0, 1, pl.ds(t, 1)] = va[t, pl.ds(top, 1)]
    exchange(0)

    def edge_sends(a, ref, off):
        for d, (peer, t) in enumerate(((lower, 0), (upper, tiles - 1))):
            for side, row in ((0, 0), (1, layers - WINDOW)):
                pltpu.make_async_remote_copy(
                    src_ref=ref.at[t, pl.ds(off + row, WINDOW)],
                    dst_ref=hedge.at[d, a, side],
                    send_sem=h_send.at[0],
                    recv_sem=h_recv.at[0, d],
                    device_id=(b, peer),
                    device_id_type=MESH,
                ).start()

    edge_sends(0, va, SUB)
    for d, (peer, t) in enumerate(((lower, 0), (upper, tiles - 1))):
        pltpu.make_async_remote_copy(
            src_ref=proj_ref.at[:, pl.ds(t * LANES, LANES)],
            dst_ref=hproj.at[d],
            send_sem=h_send.at[1],
            recv_sem=h_recv.at[1, d],
            device_id=(b, peer),
            device_id_type=MESH,
        ).start()
    for c in loads[tiles:]:
        c.wait()
    edge_sends(1, heat, 0)
    edge_sends(2, cond, 0)

    lane_block = lax.broadcasted_iota(jnp.int32, (LANES, LANES), 1)

    def packing(i, _):
        at = pl.multiple_of(i * LANES, LANES)
        rows = pl.ds(at, LANES)
        s_rows = pl.ds(pl.multiple_of(at + SUB, SUB), LANES)
        s0, s1 = va[0, s_rows], va[tiles - 1, s_rows]
        h0, h1 = heat[0, rows], heat[tiles - 1, rows]
        c0, c1 = cond[0, rows], cond[tiles - 1, rows]
        x = pltpu.roll(c1, 64, 1)
        x = jnp.where(lane_block < 56, pltpu.roll(h1, 56, 1), x)
        x = jnp.where(lane_block < 48, pltpu.roll(s1, 48, 1), x)
        x = jnp.where(lane_block < 32, pltpu.roll(c0, 24, 1), x)
        x = jnp.where(lane_block < 24, pltpu.roll(h0, 16, 1), x)
        x = jnp.where(lane_block < 16, s0, x)
        y = x.T
        pack[0, :, rows] = y[:STRIP]
        pack[1, :, rows] = y[STRIP : 2 * STRIP]
        return 0

    lax.fori_loop(0, blocks_of_rows, packing, 0)
    strips = []
    for d, peer in enumerate((lower, upper)):
        c = pltpu.make_async_remote_copy(
            src_ref=pack.at[d],
            dst_ref=got.at[d],
            send_sem=p_send.at[d],
            recv_sem=p_recv.at[d],
            device_id=(b, peer),
            device_id_type=MESH,
        )
        c.start()
        strips.append(c)

    def inverses(i, _):
        rows = pl.ds(pl.multiple_of(i * CHUNK, CHUNK), CHUNK)
        for t in range(tiles):
            inv[t, rows] = 1.0 / (4.0 + cond[t, rows])
        return 0

    lax.fori_loop(0, layers // CHUNK, inverses, 0)

    lane_w = lax.broadcasted_iota(jnp.int32, (WINDOW, LANES), 1)
    row_w = lax.broadcasted_iota(jnp.int32, (WINDOW, LANES), 0)
    near_upper = (lane_w < 16) & has_upper
    near_lower = (lane_w >= 112) & has_lower
    for d in range(2):
        bytes_of(hedge.at[d], h_recv.at[0, d])
        bytes_of(hproj.at[d], h_recv.at[1, d])
    bytes_of(hedge, h_send.at[0])
    bytes_of(hproj, h_send.at[1])
    for side, row in ((0, 0), (1, layers - WINDOW)):
        for t in range(tiles):
            ex[side, t] = va[t, pl.ds(SUB + row, WINDOW)]
            eh[side, t] = heat[t, pl.ds(row, WINDOW)]
            ei[side, t] = inv[t, pl.ds(row, WINDOW)]

        def joined(a, f):
            r, l = f(hedge[0, a, side]), f(hedge[1, a, side])
            return jnp.where(near_upper, r, jnp.where(near_lower, l, 0.0))

        ex[side, halo] = joined(0, lambda x: x)
        eh[side, halo] = joined(1, lambda x: x)
        ei[side, halo] = joined(2, lambda x: 1.0 / (4.0 + x))

    lane_row = lax.broadcasted_iota(jnp.int32, (1, LANES), 1)
    for side in range(2):
        for t in range(tiles):
            idx[side, pl.ds(t, 1)] = proj_ref[pl.ds(side, 1), pl.ds(t * LANES, LANES)]
        idx[side, pl.ds(halo, 1)] = jnp.where(
            lane_row < 64, hproj[0, pl.ds(side, 1)], hproj[1, pl.ds(side, 1)]
        )
    sub_iota = lax.broadcasted_iota(jnp.int32, (SUB, LANES), 0)
    exists = (b > 0, b < nblk - 1)

    def ghosts(stage, side, count):
        bytes_of(seen.at[stage, side], e_recv.at[stage, side])
        for i in range(nin):
            table[pl.ds(i * tiles, tiles)] = seen[stage, side, i]
        limit = jnp.where(exists[side], counts_ref[0, side], 0)
        result = []
        for t in range(count):
            at = idx[side, pl.ds(t, 1)]
            low = jnp.broadcast_to(at & (LANES - 1), (SUB, LANES))
            high = jnp.broadcast_to(at >> 7, (SUB, LANES))
            total = jnp.zeros((SUB, LANES), F32)
            for g in range(nin * tiles // SUB):
                picked = jnp.take_along_axis(
                    table[pl.ds(g * SUB, SUB)], low, axis=1, mode="promise_in_bounds"
                )
                total = jnp.where(high == sub_iota + g * SUB, picked, total)
            row = jnp.sum(total, axis=0, keepdims=True)
            if t == halo:
                place = jnp.where(lane_row < 64, k * width + width, k * width - LANES) + lane_row
            else:
                place = k * width + t * LANES + lane_row
            result.append(jnp.where(place < limit, row, 0.0))
        return result

    def edge_stage(stage):
        sweep, colour = stage // 2, stage % 2
        mine = colour_ref[sweep, 0] == colour
        for side in range(2):
            g = ghosts(stage, side, ntiles)
            x = [ex[side, t] for t in range(ntiles)]
            old = x
            for _ in range(INNER):
                left, right = shift_lanes(x, lane_w)
                new = []
                for t in range(ntiles):
                    up = pltpu.roll(x[t], 1, 0)
                    down = pltpu.roll(x[t], WINDOW - 1, 0)
                    if side == 0:
                        up = jnp.where(row_w == 0, g[t], up)
                    else:
                        down = jnp.where(row_w == WINDOW - 1, g[t], down)
                    near = up + down + left[t] + right[t]
                    new.append((eh[side, t] + near) * ei[side, t])
                x = new
            for t in range(ntiles):
                y = jnp.where(mine, x[t], old[t])
                ex[side, t] = y
                if t < tiles:
                    if side == 0:
                        trace[stage + 1, 1, pl.ds(t, 1)] = y[:1]
                    else:
                        trace[stage + 1, 0, pl.ds(t, 1)] = y[WINDOW - 1 :]
        exchange(stage + 1)

    edge_stage(0)

    for c in strips:
        c.wait()

    def unpacking(i, _):
        at = pl.multiple_of(i * LANES, LANES)
        rows = pl.ds(at, LANES)
        x = jnp.concatenate(
            [got[0, :, rows], got[1, :, rows], jnp.zeros((LANES - 2 * STRIP, LANES), F32)], 0
        )
        z = x.T
        up16 = (lane_block < 16) & has_upper
        lo16 = (lane_block >= 112) & has_lower
        up8 = (lane_block < 8) & has_upper
        lo8 = (lane_block >= 120) & has_lower
        va[halo, pl.ds(pl.multiple_of(at + SUB, SUB), LANES)] = jnp.where(
            up16, z, jnp.where(lo16, pltpu.roll(z, 80, 1), 0.0)
        )
        heat[halo, rows] = jnp.where(
            up8, pltpu.roll(z, 112, 1), jnp.where(lo8, pltpu.roll(z, 72, 1), 0.0)
        )
        c = jnp.where(up8, pltpu.roll(z, 104, 1), pltpu.roll(z, 64, 1))
        inv[halo, rows] = jnp.where(up8 | lo8, 1.0 / (4.0 + c), 0.0)
        return 0

    lax.fori_loop(0, blocks_of_rows, unpacking, 0)

    lane_c = lax.broadcasted_iota(jnp.int32, (CHUNK, LANES), 1)

    def step(old, new):
        def body(i, _):
            at = pl.multiple_of(i * CHUNK, CHUNK)
            rows = pl.ds(at, CHUNK)
            mid = pl.ds(pl.multiple_of(at + SUB, SUB), CHUNK)
            x = [old[t, mid] for t in range(ntiles)]
            left, right = shift_lanes(x, lane_c)
            for t in range(ntiles):
                up = old[t, pl.ds(at + SUB - 1, CHUNK)]
                down = old[t, pl.ds(at + SUB + 1, CHUNK)]
                near = up + down + left[t] + right[t]
                new[t, mid] = (heat[t, rows] + near) * inv[t, rows]
            return 0

        lax.fori_loop(0, layers // CHUNK, body, 0)

    for stage in range(1, 2 * SWEEPS):
        step(va, vb)
        step(vb, va)
        edge_stage(stage)
    step(va, vb)
    step(vb, va)

    for side, row, off in ((0, 0, 0), (1, layers - SUB, WINDOW - SUB)):
        for t in range(ntiles):
            va[t, pl.ds(SUB + row, SUB)] = ex[side, t, pl.ds(off, SUB)]

    def misfit(row, size, lane, ghost=None):
        rows = pl.ds(row, size)
        mid = pl.ds(row + SUB, size)
        x = [va[t, mid] for t in range(ntiles)]
        left, right = shift_lanes(x, lane)
        total = None
        for t in range(tiles):
            out_ref[rows, pl.ds(t * LANES, LANES)] = x[t]
            up = va[t, pl.ds(row + SUB - 1, size)]
            down = va[t, pl.ds(row + SUB + 1, size)]
            if ghost is not None:
                side, g = ghost
                if side == 0:
                    up = jnp.where(sub_iota == 0, g[t], up)
                else:
                    down = jnp.where(sub_iota == SUB - 1, g[t], down)
            near = up + down + left[t] + right[t]
            r = heat[t, rows] - ((4.0 + cond[t, rows]) * x[t] - near)
            r = r * r
            total = r if total is None else total + r
        return jnp.sum(total.reshape(size // SUB, SUB, LANES), axis=0)

    size = SUB * 10
    lane_m = lax.broadcasted_iota(jnp.int32, (size, LANES), 1)
    lane_s = lax.broadcasted_iota(jnp.int32, (SUB, LANES), 1)

    def residual(i, total):
        return total + misfit(pl.multiple_of(i * size + SUB, SUB), size, lane_m)

    total = lax.fori_loop(0, (layers - 2 * SUB) // size, residual, jnp.zeros((SUB, LANES), F32))
    rest = SUB + (layers - 2 * SUB) // size * size
    while rest < layers - SUB:
        total = total + misfit(rest, SUB, lane_s)
        rest += SUB
    final = 2 * SWEEPS
    total = total + misfit(0, SUB, lane_s, (0, ghosts(final, 0, tiles)))
    total = total + misfit(layers - SUB, SUB, lane_s, (1, ghosts(final, 1, tiles)))

    mine = jnp.sum(total, axis=0, keepdims=True)
    part[...] = mine

    def share(i, _):
        pltpu.make_async_remote_copy(
            src_ref=part,
            dst_ref=parts.at[k],
            send_sem=s_send,
            recv_sem=s_recv,
            device_id=(b, lax.rem(k + i, nin)),
            device_id_type=MESH,
        ).start()
        return 0

    lax.fori_loop(1, nin, share, 0)
    for stage in range(2 * SWEEPS + 1):
        bytes_of(seen.at[stage], e_send.at[stage])
    parts[k] = mine
    bytes_of(parts.at[pl.ds(0, nin - 1)], s_recv)
    bytes_of(parts.at[pl.ds(0, nin - 1)], s_send)
    whole = parts[0]
    for i in range(1, nin):
        whole = whole + parts[i]
    whole = jnp.sum(whole, axis=1, keepdims=True)
    rms = jnp.sqrt(jnp.broadcast_to(whole, (SUB, LANES)) / (layers * width * nin) + 1e-6)
    rms_ref[0] = rms[0, 0]


def solution(mesh):
    nblk, nin = mesh.shape["blk"], mesh.shape["in"]

    def per_device(heat_source, conductance, start_field, colour_map, projection, face_counts):
        layers, width = start_field.shape
        tiles = width // LANES
        n = tiles + 1
        stages = 2 * SWEEPS + 1
        vmem, smem = pltpu.VMEM, pltpu.SMEM
        dma = pltpu.SemaphoreType.DMA
        field, rms = pl.pallas_call(
            functools.partial(kernel, nblk, nin),
            out_shape=(
                jax.ShapeDtypeStruct((layers, width), F32),
                jax.ShapeDtypeStruct((1,), F32),
            ),
            in_specs=[
                pl.BlockSpec(memory_space=smem),
                pl.BlockSpec(memory_space=smem),
                pl.BlockSpec(memory_space=pl.ANY),
                pl.BlockSpec(memory_space=pl.ANY),
                pl.BlockSpec(memory_space=pl.ANY),
                pl.BlockSpec(memory_space=vmem),
            ],
            out_specs=(pl.BlockSpec(memory_space=vmem), pl.BlockSpec(memory_space=smem)),
            scratch_shapes=[
                vmem((n, layers + 2 * SUB, LANES), F32),
                vmem((n, layers + 2 * SUB, LANES), F32),
                vmem((n, layers, LANES), F32),
                vmem((tiles, layers, LANES), F32),
                vmem((n, layers, LANES), F32),
                vmem((2, STRIP, layers), F32),
                vmem((2, STRIP, layers), F32),
                vmem((2, 3, 2, WINDOW, LANES), F32),
                vmem((2, 2, LANES), jnp.int32),
                vmem((stages, 2, tiles, LANES), F32),
                vmem((stages, 2, nin, tiles, LANES), F32),
                vmem((nin * tiles, LANES), F32),
                vmem((2, SUB, LANES), jnp.int32),
                vmem((2, n, WINDOW, LANES), F32),
                vmem((2, n, WINDOW, LANES), F32),
                vmem((2, n, WINDOW, LANES), F32),
                vmem((1, LANES), F32),
                vmem((nin, 1, LANES), F32),
                dma((3, tiles)),
                dma((stages,)),
                dma((stages, 2)),
                dma((2,)),
                dma((2, 2)),
                dma((2,)),
                dma((2,)),
                dma,
                dma,
            ],
            compiler_params=pltpu.CompilerParams(
                collective_id=0, has_side_effects=True, vmem_limit_bytes=40 * 1024 * 1024
            ),
        )(
            colour_map, face_counts, heat_source, conductance, start_field,
            projection.reshape(projection.shape[1:]),
        )
        return field, rms

    placed = (
        P("blk", "in"),
        P("blk", "in"),
        P("blk", "in"),
        P(None, "blk"),
        P("blk", None, "in"),
        P("blk", None),
    )
    return jax.shard_map(
        per_device,
        mesh=mesh,
        in_specs=placed,
        out_specs=(P("blk", "in"), P("blk")),
        check_vma=False,
    )
```

```python
import functools

import jax
import jax.numpy as jnp
from jax import lax
from jax.experimental import pallas as pl
from jax.experimental.pallas import tpu as pltpu
from jax.sharding import PartitionSpec as P

SWEEPS = 2
INNER = 4
LANES = 128
SUB = 8
WINDOW = 16
STRIP = 32
CHUNK = 256
MESH = pl.DeviceIdType.MESH
F32 = jnp.float32


def shift_lanes(tiles, lane):
    n = len(tiles)
    fwd = [pltpu.roll(x, 1, 1) for x in tiles]
    back = [pltpu.roll(x, LANES - 1, 1) for x in tiles]
    left = [jnp.where(lane == 0, fwd[(t - 1) % n], fwd[t]) for t in range(n)]
    right = [jnp.where(lane == LANES - 1, back[(t + 1) % n], back[t]) for t in range(n)]
    return left, right


def kernel(
    nblk, nin, colour_hbm, counts_hbm, heat_hbm, cond_hbm, start_hbm, proj_hbm,
    out_ref, rms_ref,
    colour_ref, counts_ref, proj_ref,
    va, vb, heat, cond, inv, pack, got, hedge, hproj, trace, seen, table, idx, ex, eh, ei,
    part, parts,
    load_sem, small_sem, e_send, e_recv, h_send, h_recv, p_send, p_recv, s_send, s_recv,
):
    layers, width = start_hbm.shape
    tiles = width // LANES
    halo = tiles
    ntiles = tiles + 1
    blocks_of_rows = layers // LANES
    b = lax.axis_index("blk")
    k = lax.axis_index("in")
    before, after = lax.rem(b + nblk - 1, nblk), lax.rem(b + 1, nblk)
    lower, upper = lax.rem(k + nin - 1, nin), lax.rem(k + 1, nin)
    has_lower, has_upper = k > 0, k < nin - 1
    has_before, has_after = b > 0, b < nblk - 1
    top = SUB
    last = SUB + layers - 1

    loads = []
    for a, (src, dst, off) in enumerate(
        ((start_hbm, va, SUB), (heat_hbm, heat, 0), (cond_hbm, cond, 0))
    ):
        for t in range(tiles):
            c = pltpu.make_async_copy(
                src.at[:, pl.ds(t * LANES, LANES)],
                dst.at[t, pl.ds(off, layers)],
                load_sem.at[a, t],
            )
            c.start()
            loads.append(c)
    small = []
    for i, (src, dst) in enumerate(
        ((proj_hbm, proj_ref), (colour_hbm, colour_ref), (counts_hbm, counts_ref))
    ):
        c = pltpu.make_async_copy(src, dst, small_sem.at[i])
        c.start()
        small.append(c)

    barrier = pltpu.get_barrier_semaphore()

    def greet(i, _):
        for block in (before, after):
            pl.semaphore_signal(barrier, inc=1, device_id=(block, i), device_id_type=MESH)
        return 0

    def greet_own(i, _):
        pl.semaphore_signal(
            barrier, inc=1, device_id=(b, lax.rem(k + i, nin)), device_id_type=MESH
        )
        return 0

    lax.fori_loop(0, nin, greet, 0)
    lax.fori_loop(1, nin, greet_own, 0)

    zeros = jnp.zeros((SUB, LANES), F32)
    for v in (va, vb):
        for t in range(ntiles):
            v[t, pl.ds(0, SUB)] = zeros
            v[t, pl.ds(SUB + layers, SUB)] = zeros

    for c in loads:
        c.wait()

    lane_block = lax.broadcasted_iota(jnp.int32, (LANES, LANES), 1)

    def packing(i, _):
        at = pl.multiple_of(i * LANES, LANES)
        rows = pl.ds(at, LANES)
        s_rows = pl.ds(pl.multiple_of(at + SUB, SUB), LANES)
        s0, s1 = va[0, s_rows], va[tiles - 1, s_rows]
        h0, h1 = heat[0, rows], heat[tiles - 1, rows]
        c0, c1 = cond[0, rows], cond[tiles - 1, rows]
        x = pltpu.roll(c1, 64, 1)
        x = jnp.where(lane_block < 56, pltpu.roll(h1, 56, 1), x)
        x = jnp.where(lane_block < 48, pltpu.roll(s1, 48, 1), x)
        x = jnp.where(lane_block < 32, pltpu.roll(c0, 24, 1), x)
        x = jnp.where(lane_block < 24, pltpu.roll(h0, 16, 1), x)
        x = jnp.where(lane_block < 16, s0, x)
        y = x.T
        pack[0, :, rows] = y[:STRIP]
        pack[1, :, rows] = y[STRIP : 2 * STRIP]
        return 0

    lax.fori_loop(0, blocks_of_rows, packing, 0)
    def inverses(i, _):
        rows = pl.ds(pl.multiple_of(i * CHUNK, CHUNK), CHUNK)
        for t in range(tiles):
            inv[t, rows] = 1.0 / (4.0 + cond[t, rows])
        return 0

    lax.fori_loop(0, layers // CHUNK, inverses, 0)

    pl.semaphore_wait(barrier, 3 * nin - 1)

    def exchange(stage):
        for side, block, there in ((0, after, has_after), (1, before, has_before)):

            @pl.when(there)
            def _():
                def send(i, _):
                    pltpu.make_async_remote_copy(
                        src_ref=trace.at[stage, side],
                        dst_ref=seen.at[stage, side, k],
                        send_sem=e_send.at[stage, side],
                        recv_sem=e_recv.at[stage, side],
                        device_id=(block, i),
                        device_id_type=MESH,
                    ).start()
                    return 0

                lax.fori_loop(0, nin, send, 0)

    def bytes_of(ref, sem):
        pltpu.make_async_copy(ref, ref, sem).wait()

    for t in range(tiles):
        trace[0, 0, pl.ds(t, 1)] = va[t, pl.ds(last, 1)]
        trace[0, 1, pl.ds(t, 1)] = va[t, pl.ds(top, 1)]
    exchange(0)

    for c in small:
        c.wait()
    sides = ((lower, 0, has_lower), (upper, tiles - 1, has_upper))

    def strip(d, peer):
        return pltpu.make_async_remote_copy(
            src_ref=pack.at[d],
            dst_ref=got.at[d],
            send_sem=p_send.at[d],
            recv_sem=p_recv.at[d],
            device_id=(b, peer),
            device_id_type=MESH,
        )

    for d, (peer, t, there) in enumerate(sides):

        @pl.when(there)
        def _():
            for a, (ref, off) in enumerate(((va, SUB), (heat, 0), (cond, 0))):
                for side, row in ((0, 0), (1, layers - WINDOW)):
                    pltpu.make_async_remote_copy(
                        src_ref=ref.at[t, pl.ds(off + row, WINDOW)],
                        dst_ref=hedge.at[d, a, side],
                        send_sem=h_send.at[0, d],
                        recv_sem=h_recv.at[0, d],
                        device_id=(b, peer),
                        device_id_type=MESH,
                    ).start()
            pltpu.make_async_remote_copy(
                src_ref=proj_ref.at[:, pl.ds(t * LANES, LANES)],
                dst_ref=hproj.at[d],
                send_sem=h_send.at[1, d],
                recv_sem=h_recv.at[1, d],
                device_id=(b, peer),
                device_id_type=MESH,
            ).start()
            strip(d, peer).start()

    lane_w = lax.broadcasted_iota(jnp.int32, (WINDOW, LANES), 1)
    row_w = lax.broadcasted_iota(jnp.int32, (WINDOW, LANES), 0)
    near_upper = (lane_w < 16) & has_upper
    near_lower = (lane_w >= 112) & has_lower
    for d, there in ((0, has_upper), (1, has_lower)):

        @pl.when(there)
        def _():
            bytes_of(hedge.at[d], h_recv.at[0, d])
            bytes_of(hproj.at[d], h_recv.at[1, d])

    for side, row in ((0, 0), (1, layers - WINDOW)):
        for t in range(tiles):
            ex[side, t] = va[t, pl.ds(SUB + row, WINDOW)]
            eh[side, t] = heat[t, pl.ds(row, WINDOW)]
            ei[side, t] = inv[t, pl.ds(row, WINDOW)]

        def joined(a, f):
            r, l = f(hedge[0, a, side]), f(hedge[1, a, side])
            return jnp.where(near_upper, r, jnp.where(near_lower, l, 0.0))

        ex[side, halo] = joined(0, lambda x: x)
        eh[side, halo] = joined(1, lambda x: x)
        ei[side, halo] = joined(2, lambda x: 1.0 / (4.0 + x))

    lane_row = lax.broadcasted_iota(jnp.int32, (1, LANES), 1)
    for side in range(2):
        for t in range(tiles):
            idx[side, pl.ds(t, 1)] = proj_ref[pl.ds(side, 1), pl.ds(t * LANES, LANES)]
        idx[side, pl.ds(halo, 1)] = jnp.where(
            lane_row < 64, hproj[0, pl.ds(side, 1)], hproj[1, pl.ds(side, 1)]
        )
    sub_iota = lax.broadcasted_iota(jnp.int32, (SUB, LANES), 0)
    exists = (has_before, has_after)

    def ghosts(stage, side, count):
        @pl.when(exists[side])
        def _():
            bytes_of(seen.at[stage, side], e_recv.at[stage, side])

        for i in range(nin):
            table[pl.ds(i * tiles, tiles)] = seen[stage, side, i]
        limit = jnp.where(exists[side], counts_ref[0, side], 0)
        result = []
        for t in range(count):
            at = idx[side, pl.ds(t, 1)]
            low = jnp.broadcast_to(at & (LANES - 1), (SUB, LANES))
            high = jnp.broadcast_to(at >> 7, (SUB, LANES))
            total = jnp.zeros((SUB, LANES), F32)
            for g in range(nin * tiles // SUB):
                picked = jnp.take_along_axis(
                    table[pl.ds(g * SUB, SUB)], low, axis=1, mode="promise_in_bounds"
                )
                total = jnp.where(high == sub_iota + g * SUB, picked, total)
            row = jnp.sum(total, axis=0, keepdims=True)
            if t == halo:
                place = jnp.where(lane_row < 64, k * width + width, k * width - LANES) + lane_row
            else:
                place = k * width + t * LANES + lane_row
            result.append(jnp.where(place < limit, row, 0.0))
        return result

    def edge_stage(stage):
        sweep, colour = stage // 2, stage % 2
        mine = colour_ref[0, sweep] == colour
        for side in range(2):
            g = ghosts(stage, side, ntiles)
            x = [ex[side, t] for t in range(ntiles)]
            old = x
            for _ in range(INNER):
                left, right = shift_lanes(x, lane_w)
                new = []
                for t in range(ntiles):
                    up = pltpu.roll(x[t], 1, 0)
                    down = pltpu.roll(x[t], WINDOW - 1, 0)
                    if side == 0:
                        up = jnp.where(row_w == 0, g[t], up)
                    else:
                        down = jnp.where(row_w == WINDOW - 1, g[t], down)
                    near = up + down + left[t] + right[t]
                    new.append((eh[side, t] + near) * ei[side, t])
                x = new
            for t in range(ntiles):
                y = jnp.where(mine, x[t], old[t])
                ex[side, t] = y
                if t < tiles:
                    if side == 0:
                        trace[stage + 1, 1, pl.ds(t, 1)] = y[:1]
                    else:
                        trace[stage + 1, 0, pl.ds(t, 1)] = y[WINDOW - 1 :]
        exchange(stage + 1)

    edge_stage(0)

    for d, there in ((0, has_upper), (1, has_lower)):

        @pl.when(there)
        def _():
            strip(d, lower).wait_recv()

    for d, (peer, t, there) in enumerate(sides):

        @pl.when(there)
        def _():
            bytes_of(hedge.at[d], h_send.at[0, d])
            bytes_of(hproj.at[d], h_send.at[1, d])


    def unpacking(i, _):
        at = pl.multiple_of(i * LANES, LANES)
        rows = pl.ds(at, LANES)
        x = jnp.concatenate(
            [got[0, :, rows], got[1, :, rows], jnp.zeros((LANES - 2 * STRIP, LANES), F32)], 0
        )
        z = x.T
        up16 = (lane_block < 16) & has_upper
        lo16 = (lane_block >= 112) & has_lower
        up8 = (lane_block < 8) & has_upper
        lo8 = (lane_block >= 120) & has_lower
        va[halo, pl.ds(pl.multiple_of(at + SUB, SUB), LANES)] = jnp.where(
            up16, z, jnp.where(lo16, pltpu.roll(z, 80, 1), 0.0)
        )
        heat[halo, rows] = jnp.where(
            up8, pltpu.roll(z, 112, 1), jnp.where(lo8, pltpu.roll(z, 72, 1), 0.0)
        )
        c = jnp.where(up8, pltpu.roll(z, 104, 1), pltpu.roll(z, 64, 1))
        inv[halo, rows] = jnp.where(up8 | lo8, 1.0 / (4.0 + c), 0.0)
        return 0

    lax.fori_loop(0, blocks_of_rows, unpacking, 0)

    lane_c = lax.broadcasted_iota(jnp.int32, (CHUNK, LANES), 1)

    def step(old, new):
        def body(i, _):
            at = pl.multiple_of(i * CHUNK, CHUNK)
            rows = pl.ds(at, CHUNK)
            mid = pl.ds(pl.multiple_of(at + SUB, SUB), CHUNK)
            x = [old[t, mid] for t in range(ntiles)]
            left, right = shift_lanes(x, lane_c)
            for t in range(ntiles):
                up = old[t, pl.ds(at + SUB - 1, CHUNK)]
                down = old[t, pl.ds(at + SUB + 1, CHUNK)]
                near = up + down + left[t] + right[t]
                new[t, mid] = (heat[t, rows] + near) * inv[t, rows]
            return 0

        lax.fori_loop(0, layers // CHUNK, body, 0)

    for stage in range(1, 2 * SWEEPS):
        step(va, vb)
        step(vb, va)
        edge_stage(stage)
    step(va, vb)
    step(vb, va)

    for side, row, off in ((0, 0, 0), (1, layers - SUB, WINDOW - SUB)):
        for t in range(ntiles):
            va[t, pl.ds(SUB + row, SUB)] = ex[side, t, pl.ds(off, SUB)]

    def misfit(row, size, lane, ghost=None):
        rows = pl.ds(row, size)
        mid = pl.ds(row + SUB, size)
        x = [va[t, mid] for t in range(ntiles)]
        left, right = shift_lanes(x, lane)
        total = None
        for t in range(tiles):
            out_ref[rows, pl.ds(t * LANES, LANES)] = x[t]
            up = va[t, pl.ds(row + SUB - 1, size)]
            down = va[t, pl.ds(row + SUB + 1, size)]
            if ghost is not None:
                side, g = ghost
                if side == 0:
                    up = jnp.where(sub_iota == 0, g[t], up)
                else:
                    down = jnp.where(sub_iota == SUB - 1, g[t], down)
            near = up + down + left[t] + right[t]
            r = heat[t, rows] - ((4.0 + cond[t, rows]) * x[t] - near)
            r = r * r
            total = r if total is None else total + r
        return jnp.sum(total.reshape(size // SUB, SUB, LANES), axis=0)

    size = SUB * 10
    lane_m = lax.broadcasted_iota(jnp.int32, (size, LANES), 1)
    lane_s = lax.broadcasted_iota(jnp.int32, (SUB, LANES), 1)

    def residual(i, total):
        return total + misfit(pl.multiple_of(i * size + SUB, SUB), size, lane_m)

    total = lax.fori_loop(0, (layers - 2 * SUB) // size, residual, jnp.zeros((SUB, LANES), F32))
    rest = SUB + (layers - 2 * SUB) // size * size
    while rest < layers - SUB:
        total = total + misfit(rest, SUB, lane_s)
        rest += SUB
    final = 2 * SWEEPS
    total = total + misfit(0, SUB, lane_s, (0, ghosts(final, 0, tiles)))
    total = total + misfit(layers - SUB, SUB, lane_s, (1, ghosts(final, 1, tiles)))

    mine = jnp.sum(total, axis=0, keepdims=True)
    part[...] = mine

    def share(i, _):
        pltpu.make_async_remote_copy(
            src_ref=part,
            dst_ref=parts.at[k],
            send_sem=s_send,
            recv_sem=s_recv,
            device_id=(b, lax.rem(k + i, nin)),
            device_id_type=MESH,
        ).start()
        return 0

    lax.fori_loop(1, nin, share, 0)
    for d, (peer, t, there) in enumerate(sides):

        @pl.when(there)
        def _():
            strip(d, peer).wait_send()

    for stage in range(2 * SWEEPS + 1):
        for side, there in ((0, has_after), (1, has_before)):

            @pl.when(there)
            def _():
                bytes_of(seen.at[stage, side], e_send.at[stage, side])

    parts[k] = mine
    bytes_of(parts.at[pl.ds(0, nin - 1)], s_recv)
    bytes_of(parts.at[pl.ds(0, nin - 1)], s_send)
    whole = parts[0]
    for i in range(1, nin):
        whole = whole + parts[i]
    whole = jnp.sum(whole, axis=1, keepdims=True)
    rms = jnp.sqrt(jnp.broadcast_to(whole, (SUB, LANES)) / (layers * width * nin) + 1e-6)
    rms_ref[0] = rms[0, 0]


def solution(mesh):
    nblk, nin = mesh.shape["blk"], mesh.shape["in"]

    def per_device(heat_source, conductance, start_field, colour_map, projection, face_counts):
        layers, width = start_field.shape
        tiles = width // LANES
        n = tiles + 1
        stages = 2 * SWEEPS + 1
        vmem, smem = pltpu.VMEM, pltpu.SMEM
        dma = pltpu.SemaphoreType.DMA
        field, rms = pl.pallas_call(
            functools.partial(kernel, nblk, nin),
            out_shape=(
                jax.ShapeDtypeStruct((layers, width), F32),
                jax.ShapeDtypeStruct((1,), F32),
            ),
            in_specs=[pl.BlockSpec(memory_space=pltpu.HBM)] * 6,
            out_specs=(pl.BlockSpec(memory_space=vmem), pl.BlockSpec(memory_space=smem)),
            scratch_shapes=[
                smem((1, SWEEPS), jnp.int32),
                smem((1, 2), jnp.int32),
                vmem((2, width), jnp.int32),
                vmem((n, layers + 2 * SUB, LANES), F32),
                vmem((n, layers + 2 * SUB, LANES), F32),
                vmem((n, layers, LANES), F32),
                vmem((tiles, layers, LANES), F32),
                vmem((n, layers, LANES), F32),
                vmem((2, STRIP, layers), F32),
                vmem((2, STRIP, layers), F32),
                vmem((2, 3, 2, WINDOW, LANES), F32),
                vmem((2, 2, LANES), jnp.int32),
                vmem((stages, 2, tiles, LANES), F32),
                vmem((stages, 2, nin, tiles, LANES), F32),
                vmem((nin * tiles, LANES), F32),
                vmem((2, SUB, LANES), jnp.int32),
                vmem((2, n, WINDOW, LANES), F32),
                vmem((2, n, WINDOW, LANES), F32),
                vmem((2, n, WINDOW, LANES), F32),
                vmem((1, LANES), F32),
                vmem((nin, 1, LANES), F32),
                dma((3, tiles)),
                dma((3,)),
                dma((stages, 2)),
                dma((stages, 2)),
                dma((2, 2)),
                dma((2, 2)),
                dma((2,)),
                dma((2,)),
                dma,
                dma,
            ],
            compiler_params=pltpu.CompilerParams(
                collective_id=0, has_side_effects=True, vmem_limit_bytes=65 * 1000 * 1000
            ),
        )(
            colour_map.T, face_counts, heat_source, conductance, start_field,
            projection.reshape(projection.shape[1:]),
        )
        return field, rms

    placed = (
        P("blk", "in"),
        P("blk", "in"),
        P("blk", "in"),
        P(None, "blk"),
        P("blk", None, "in"),
        P("blk", None),
    )
    return jax.shard_map(
        per_device,
        mesh=mesh,
        in_specs=placed,
        out_specs=(P("blk", "in"), P("blk")),
        check_vma=False,
    )
```
